512 devices in a mesh: graph: 128 (over z, y, core), member: 4 (over x).
Axes of the slice: x: 4, y: 8, z: 8, core: 2. Of those that a mesh axis runs over, the one named last changes fastest.
Arguments:
- node_latents: bfloat16 [16, 16384, 512], P('member', 'graph'), may hold values from -6 to 6
- edge_latents: bfloat16 [98304, 512], P('graph'), may hold values from -6 to 6
- neighbours: int32 [128, 4], P('graph'), may hold values from 0 to 127, as said below
- edge_source: int32 [128, 768], P('graph'), may hold values from 0 to 639, as said below
- edge_dest: int32 [128, 768], P('graph'), may hold values from 0 to 127, as said below
- edge_count: int32 [128], P('graph'), may hold values from 153 to 768, as said below
- edge_in: bfloat16 [1, 3, 512, 512], replicated, may hold values from -0.15625 to 0.15625
- edge_out: bfloat16 [1, 512, 512], replicated, may hold values from -0.25 to 0.25
- node_in: bfloat16 [1, 2, 512, 512], replicated, may hold values from -0.1875 to 0.1875
- node_out: bfloat16 [1, 512, 512], replicated, may hold values from -0.25 to 0.25
- biases: float32 [1, 4, 512], replicated, may hold values from -3 to 3
- gains: float32 [1, 2, 512], replicated, may hold values from 0.25 to 1.75
Outputs:
- ens_mean: bfloat16 [16384, 512], P('graph')
- ens_spread: bfloat16 [16384, 512], P('graph')
The draws below stay inside these ranges and needn't reach their ends.
Inputs may be any that keep to these rules, and one draw needn't show every extreme that they name: `neighbours`: row b lists 4 distinct blocks other than b, each within 3 blocks of b along the closed order of blocks (numbers taken modulo 128). `edge_source`: among the live edge slots of one block, at most 32 distinct sender nodes lie in any one listed block, and exactly 32 in one of them. `edge_dest`: every node receives at least one live edge slot of its block. `edge_count`: some block has all 768 slots live.
All inputs are finite; a program needn't handle non-finite values.
Results may differ from the reference program's by a relative error of at most 0.006.
Values may be sent and summed in bfloat16 or wider, within the bound.
A program may use at most 64 MiB of HBM per device.

```python
import jax
import jax.numpy as jnp
from jax import lax

L = 512
BLK = 128
EDGE_DEV = 768
NBRS = 4
RADIUS = 3
CAP = 32
LAYERS = 1
BLOCKS = 128
NODES = 16384
EDGES = 98304
MEMBERS = 16


def graph_tables(key):
    folded = jax.random.fold_in(key, 4242)
    keys = jax.random.split(folded, 8)
    blocks = jnp.arange(BLOCKS, dtype=jnp.int32)
    candidate_ids = jnp.arange(2 * RADIUS, dtype=jnp.int32)
    candidates = jnp.where(candidate_ids < RADIUS, candidate_ids + 1, RADIUS - 1 - candidate_ids)
    order = jax.vmap(lambda subkey: jax.random.permutation(subkey, 2 * RADIUS))(jax.random.split(keys[0], BLOCKS))[:, :NBRS]
    offsets = candidates[order]
    neighbours = (blocks[:, None] + offsets) % BLOCKS
    counts = EDGE_DEV // (1 + jax.random.randint(keys[1], (BLOCKS,), 0, 5))
    busiest = jax.random.randint(keys[2], (), 0, BLOCKS)
    counts = jnp.where(blocks == busiest, EDGE_DEV, counts)
    needed = jax.random.randint(keys[3], (BLOCKS, NBRS), CAP // 2, CAP + 1)
    widest = jax.random.randint(keys[4], (BLOCKS,), 0, NBRS)
    needed = jnp.where(jnp.arange(NBRS, dtype=jnp.int32)[None, :] == widest[:, None], CAP, needed)
    chosen = jax.vmap(lambda subkey: jax.random.permutation(subkey, BLK))(jax.random.split(keys[5], BLOCKS * NBRS))
    chosen = chosen.reshape(BLOCKS, NBRS, BLK)[:, :, :CAP].reshape(BLOCKS, NBRS * CAP)
    slots = jnp.arange(EDGE_DEV, dtype=jnp.int32)
    first_slot = jnp.minimum(slots // CAP, NBRS - 1)
    first_rank = slots % CAP
    in_first = (slots < NBRS * CAP)[None, :]
    random_bits = jax.random.randint(keys[6], (4, BLOCKS, EDGE_DEV), 0, 1 << 20)
    slot_pick = jnp.where(in_first, first_slot[None, :], random_bits[0] % NBRS)
    need_at = jnp.take_along_axis(needed, slot_pick, axis=1)
    rank_pick = jnp.where(in_first, first_rank[None, :], random_bits[1] % need_at)
    remote = jnp.where(in_first, first_rank[None, :] < need_at, random_bits[2] % 4 == 0)
    node_pick = jnp.take_along_axis(chosen, slot_pick * CAP + rank_pick, axis=1)
    own_node = random_bits[3] % BLK
    source = jnp.where(remote, slot_pick * BLK + node_pick, NBRS * BLK + own_node)
    receivers = jax.vmap(lambda subkey: jax.random.permutation(subkey, BLK))(jax.random.split(keys[7], BLOCKS))
    dest = jnp.take(receivers, slots % BLK, axis=1)
    return (neighbours.astype(jnp.int32), source.astype(jnp.int32), dest.astype(jnp.int32), counts.astype(jnp.int32))


def draw_neighbours(key, part):
    return graph_tables(key)[0]


def draw_edge_source(key, part):
    return graph_tables(key)[1]


def draw_edge_dest(key, part):
    return graph_tables(key)[2]


def draw_edge_count(key, part):
    return graph_tables(key)[3]


def level_of(stream_key, extent, pieces, least, top_value):
    factor_of, own = 1.0, jax.random.fold_in(stream_key, 6)
    for position, blocks in pieces:
        heights = jnp.exp(jax.random.uniform(jax.random.fold_in(own, position), (blocks,), jnp.float32, least / len(pieces), top_value / len(pieces)))
        factor_of = factor_of * jnp.repeat(heights, extent[position] // blocks).reshape([-1 if axis == position else 1 for axis in range(len(extent))])
    return factor_of


def normal_values(stream_key, shape, scale, limit, shards=(), held_as=jnp.bfloat16):
    factor_of = level_of(stream_key, shape, shards, -0.22, 0.18) if shards else 1.0
    entries = jax.random.normal(stream_key, shape, jnp.float32) * scale * factor_of
    return jnp.minimum(jnp.maximum(entries, -limit), limit).astype(held_as)


def setup_inputs(seed: int = 0) -> dict:
    key_of = jax.random.split(jax.random.key(seed), 13)
    node_latents = normal_values(key_of[0], (MEMBERS, NODES, L), 1.0, 6.0, ((0, 4), (1, 128)))
    edge_latents = normal_values(key_of[1], (EDGES, L), 1.0, 6.0, ((0, 128),))
    neighbours = draw_neighbours(jax.random.fold_in(key_of[12], 71), 0)
    edge_source = draw_edge_source(jax.random.fold_in(key_of[12], 71), 0)
    edge_dest = draw_edge_dest(jax.random.fold_in(key_of[12], 71), 0)
    edge_count = draw_edge_count(jax.random.fold_in(key_of[12], 71), 0)
    edge_in = normal_values(key_of[6], (LAYERS, 3, L, L), (3 * L) ** -0.5, 0.15625)
    edge_out = normal_values(key_of[7], (LAYERS, L, L), L ** -0.5, 0.25)
    node_in = normal_values(key_of[8], (LAYERS, 2, L, L), (2 * L) ** -0.5, 0.1875)
    node_out = normal_values(key_of[9], (LAYERS, L, L), L ** -0.5, 0.25)
    biases = normal_values(key_of[10], (LAYERS, 4, L), 0.5, 3.0, (), jnp.float32)
    gains = jnp.clip(1.0 + 0.15 * jax.random.normal(key_of[11], (LAYERS, 2, L), jnp.float32), 0.25, 1.75)
    return dict(node_latents=node_latents, edge_latents=edge_latents, neighbours=neighbours, edge_source=edge_source, edge_dest=edge_dest, edge_count=edge_count, edge_in=edge_in, edge_out=edge_out, node_in=node_in, node_out=node_out, biases=biases, gains=gains)


def layer_norm(values, gain):
    centre = lax.optimization_barrier(jnp.mean(values, axis=-1, keepdims=True))
    centered = values - centre
    variance = lax.optimization_barrier(jnp.mean(centered * centered, axis=-1, keepdims=True))
    return centered * lax.rsqrt(variance + 1e-05) * gain

def reference(node_latents, edge_latents, neighbours, edge_source, edge_dest, edge_count, edge_in, edge_out, node_in, node_out, biases, gains):
    blocks = jnp.arange(BLOCKS, dtype=jnp.int32)[:, None]
    src_slot = edge_source // BLK
    src_node = edge_source % BLK
    listed = jnp.take_along_axis(neighbours, jnp.minimum(src_slot, NBRS - 1), axis=1)
    owner = jnp.where(src_slot == NBRS, blocks, listed)
    src_global = (owner * BLK + src_node).reshape(-1).astype(jnp.int32)
    dst_global = (blocks * BLK + edge_dest).reshape(-1).astype(jnp.int32)
    is_live = (jnp.arange(EDGE_DEV, dtype=jnp.int32)[None, :] < edge_count[:, None]).reshape(-1)

    def one_member(state):
        edge_state = edge_latents
        for layer_id in range(LAYERS):
            sender_proj = jnp.dot(state, edge_in[layer_id, 1], preferred_element_type=jnp.float32).astype(jnp.bfloat16)
            receiver_proj = jnp.dot(state, edge_in[layer_id, 2], preferred_element_type=jnp.float32)
            hidden = jnp.dot(edge_state, edge_in[layer_id, 0], preferred_element_type=jnp.float32)
            hidden = hidden + sender_proj[src_global].astype(jnp.float32) + receiver_proj[dst_global] + biases[layer_id, 0]
            activated = jax.nn.silu(hidden).astype(jnp.bfloat16)
            mixed = jnp.dot(activated, edge_out[layer_id], preferred_element_type=jnp.float32) + biases[layer_id, 1]
            edge_state = (edge_state.astype(jnp.float32) + layer_norm(mixed, gains[layer_id, 0])).astype(jnp.bfloat16)
            masked = jnp.where(is_live[:, None], edge_state.astype(jnp.float32), jnp.float32(0.0))
            gathered = jax.ops.segment_sum(masked, dst_global, num_segments=NODES).astype(jnp.bfloat16)
            node_hidden = jnp.dot(state, node_in[layer_id, 0], preferred_element_type=jnp.float32)
            node_hidden = node_hidden + jnp.dot(gathered, node_in[layer_id, 1], preferred_element_type=jnp.float32) + biases[layer_id, 2]
            node_act = jax.nn.silu(node_hidden).astype(jnp.bfloat16)
            node_mixed = jnp.dot(node_act, node_out[layer_id], preferred_element_type=jnp.float32) + biases[layer_id, 3]
            state = (state.astype(jnp.float32) + layer_norm(node_mixed, gains[layer_id, 1])).astype(jnp.bfloat16)
        return state
    finals = lax.map(one_member, node_latents).astype(jnp.float32)
    centre = lax.optimization_barrier(jnp.sum(finals, axis=0)) / MEMBERS
    deviation = finals - centre
    spread = jnp.sqrt(lax.optimization_barrier(jnp.sum(deviation * deviation, axis=0)) / MEMBERS)
    return (centre.astype(jnp.bfloat16), spread.astype(jnp.bfloat16))
```

```python
import jax
import jax.numpy as jnp
from jax import lax
from jax.experimental import pallas as pl
from jax.experimental.pallas import tpu as pltpu
from jax.sharding import PartitionSpec as P

RADIUS = 3
CAP = 32
EPS = 1e-05
MESH = pl.DeviceIdType.MESH
F32 = jnp.float32
BF16 = jnp.bfloat16
OFFSETS = tuple(range(1, RADIUS + 1)) + tuple(-r for r in range(1, RADIUS + 1))


def dot_nn(a, b):
    return lax.dot_general(a, b, (((1,), (0,)), ((), ())), preferred_element_type=F32)


def dot_nt(a, b):
    return lax.dot_general(a, b, (((1,), (1,)), ((), ())), preferred_element_type=F32)


def normed(values, gain):
    mean = jnp.mean(values, axis=-1, keepdims=True)
    cen = values - mean
    var = jnp.mean(cen * cen, axis=-1, keepdims=True)
    return cen * lax.rsqrt(var + EPS) * gain


def make_kernel(groups, peers, members, blk, slots, width, nbrs, layouts):
    near = len(OFFSETS)
    halo = near * CAP
    rows = blk // peers
    chunk = 256
    halo_at = 2 * blk

    def kernel(
        node_hbm, edge_hbm, nbr_hbm, src_hbm, dst_hbm, cnt_hbm,
        win_hbm, wout_hbm, nin_hbm, nout_hbm, bias_hbm, gain_hbm,
        mean_ref, spread_ref,
        node_v, edge_v, win_v, wout_v, nin_v, nout_v, bias_v, gain_v,
        src_v, dst_v, nbr_s, cnt_s,
        ask_out, ask_in, table, outbox, hot, eproj, nproj, dhot, fin, pool, result,
        in_sems, ask_ssem, ask_rsem, row_ssem, row_rsem, fin_ssem, fin_rsem, res_ssem, res_rsem,
    ):
        me = lax.axis_index("graph")
        col = lax.axis_index("member")
        near_ids = [lax.rem(me + off + groups, groups) for off in OFFSETS]
        back_ids = [lax.rem(me - off + groups, groups) for off in OFFSETS]
        peer_ids = [lax.rem(col + d, peers) for d in range(1, peers)]

        barrier = pltpu.get_barrier_semaphore()
        for g in near_ids:
            pl.semaphore_signal(barrier, inc=1, device_id={"graph": g, "member": col}, device_id_type=MESH)
        for x in peer_ids:
            pl.semaphore_signal(barrier, inc=1, device_id={"graph": me, "member": x}, device_id_type=MESH)

        loads = [
            (src_hbm, src_v), (nbr_hbm, nbr_s), (cnt_hbm, cnt_s), (dst_hbm, dst_v),
            (win_hbm.at[0, 1], win_v.at[1]), (node_hbm, node_v), (bias_hbm.at[0], bias_v), (gain_hbm.at[0], gain_v),
            (win_hbm.at[0, 2], win_v.at[2]), (nin_hbm.at[0, 0], nin_v.at[0]),
            (win_hbm.at[0, 0], win_v.at[0]), (edge_hbm, edge_v), (wout_hbm.at[0], wout_v),
            (nin_hbm.at[0, 1], nin_v.at[1]), (nout_hbm.at[0], nout_v),
        ]
        copies = [pltpu.make_async_copy(s, d, in_sems.at[i]) for i, (s, d) in enumerate(loads)]
        for c in copies:
            c.start()

        for c in copies[:4]:
            c.wait()
        lane_e = lax.broadcasted_iota(jnp.int32, (1, slots), 1)
        src = src_v[...]
        slot = src // blk
        node = src - slot * blk
        live = lane_e < cnt_s[0]
        place = jnp.full((1, slots), near, jnp.int32)
        for s in range(nbrs):
            dist = lax.rem(nbr_s[0, s] - me + groups, groups)
            p = jnp.where(dist <= RADIUS, dist - 1, RADIUS - 1 + groups - dist)
            place = jnp.where(slot == s, p, place)
        sub8 = lax.broadcasted_iota(jnp.int32, (8, slots), 0)
        subn = lax.broadcasted_iota(jnp.int32, (blk, slots), 0)
        near_hot = jnp.where((sub8 == place) & live, 1.0, 0.0).astype(BF16)
        node_hot = jnp.where(subn == node, 1.0, 0.0).astype(BF16)
        used = jnp.where(dot_nt(near_hot, node_hot) > 0.5, 1.0, 0.0)
        sq_r = lax.broadcasted_iota(jnp.int32, (blk, blk), 0)
        sq_c = lax.broadcasted_iota(jnp.int32, (blk, blk), 1)
        before = jnp.where(sq_r < sq_c, 1.0, 0.0).astype(BF16)
        rank = jnp.where(used > 0.5, dot_nn(used.astype(BF16), before), 1000.0)
        for p in range(near):
            ask_out[p] = jnp.broadcast_to(rank[p : p + 1, :], (8, blk))
        capf = lax.broadcasted_iota(jnp.int32, (CAP, blk), 0).astype(F32)
        mine = jnp.concatenate(
            [jnp.where(capf == rank[p : p + 1, :], 1.0, 0.0) for p in range(near)], axis=0
        ).astype(BF16)

        pl.semaphore_wait(barrier, near + peers - 1)

        def ask(p):
            return pltpu.make_async_remote_copy(
                src_ref=ask_out.at[p], dst_ref=ask_in.at[p], send_sem=ask_ssem.at[p], recv_sem=ask_rsem.at[p],
                device_id={"graph": near_ids[p], "member": col}, device_id_type=MESH)

        for p in range(near):
            ask(p).start()

        for c in copies[4:8]:
            c.wait()

        def project(m, carry):
            part = dot_nn(node_v[m], win_v[1])
            table[m, 0:blk, :] = (0.5 * part).astype(BF16)
            return carry

        lax.fori_loop(0, members, project, 0)

        eye = jnp.where(sq_r == sq_c, 1.0, 0.0).astype(BF16)
        lane_n = sq_c.astype(F32)
        near_of = (lax.broadcasted_iota(jnp.int32, (blk, 2 * blk), 1) // CAP).astype(F32)
        dst = dst_v[...]
        for j in range(slots // blk):
            part = slice(j * blk, (j + 1) * blk)

            def column(row, n):
                return dot_nt(eye, jnp.broadcast_to(row[:, part].astype(F32), (n, blk)).astype(BF16))

            node_c = column(node, blk)
            dst_c = column(dst, blk)
            place_c = column(place, 2 * blk)
            one = jnp.where(node_c == lane_n, 1.0, 0.0)
            hot[part, 0:blk] = jnp.where(place_c[:, 0:blk] == float(near), one, 0.0).astype(BF16)
            hot[part, blk : 2 * blk] = jnp.where(dst_c == lane_n, 1.0, 0.0).astype(BF16)
            pick = dot_nt(one.astype(BF16), mine)
            pick = jnp.concatenate([pick, jnp.zeros((blk, 2 * blk - halo), F32)], axis=1)
            hot[part, 2 * blk : 4 * blk] = jnp.where(place_c == near_of, pick, 0.0).astype(BF16)
        dhot[...] = jnp.where((subn == dst) & live, 1.0, 0.0).astype(BF16)

        for p in range(near):
            ask(p).wait_recv()
        theirs = jnp.concatenate(
            [jnp.where(capf == ask_in[p, 0:1, :], 1.0, 0.0) for p in range(near)], axis=0
        ).astype(BF16)

        def rows_to(m, p):
            return pltpu.make_async_remote_copy(
                src_ref=outbox.at[m, pl.ds(p * CAP, CAP), :],
                dst_ref=table.at[m, pl.ds(halo_at + p * CAP, CAP), :],
                send_sem=row_ssem.at[m, p], recv_sem=row_rsem.at[m, p],
                device_id={"graph": back_ids[p], "member": col}, device_id_type=MESH)

        def select(m, carry):
            outbox[m] = dot_nn(theirs, table[m, 0:blk, :]).astype(BF16)
            for p in range(near):
                rows_to(m, p).start()
            return carry

        lax.fori_loop(0, members, select, 0)

        for c in copies[8:]:
            c.wait()

        def project_more(m, carry):
            x = node_v[m]
            table[m, blk : 2 * blk, :] = (0.5 * dot_nn(x, win_v[2])).astype(BF16)
            table[m, halo_at + halo :, :] = jnp.zeros((4 * blk - halo_at - halo, width), BF16)
            nproj[m] = 0.5 * (dot_nn(x, nin_v[0]) + bias_v[2:3, :])
            return carry

        lax.fori_loop(0, members, project_more, 0)

        def project_edges(j, carry):
            part = pl.ds(pl.multiple_of(j * chunk, chunk), chunk)
            eproj[part, :] = 0.5 * (dot_nn(edge_v[part, :], win_v[0]) + bias_v[0:1, :])
            return carry

        lax.fori_loop(0, slots // chunk, project_edges, 0)

        def fin_to(m, d):
            return pltpu.make_async_remote_copy(
                src_ref=fin.at[m, pl.ds(pl.multiple_of(peer_ids[d] * rows, rows), rows), :],
                dst_ref=pool.at[col * members + m],
                send_sem=fin_ssem.at[m, d], recv_sem=fin_rsem.at[m, d],
                device_id={"graph": me, "member": peer_ids[d]}, device_id_type=MESH)

        def one_member(m, carry):
            for p in range(near):
                rows_to(m, p).wait_recv()
            total = jnp.zeros((blk, width), F32)
            for j in range(slots // chunk):
                part = slice(j * chunk, (j + 1) * chunk)
                half = dot_nn(hot[part, :], table[m]) + eproj[part, :]
                act = (half + half * jnp.tanh(half)).astype(BF16)
                mixed = dot_nn(act, wout_v[...]) + bias_v[1:2, :]
                new = (edge_v[part, :].astype(F32) + normed(mixed, gain_v[0:1, :])).astype(BF16)
                total = total + dot_nn(dhot[:, part], new)
            nhalf = 0.5 * dot_nn(total.astype(BF16), nin_v[1]) + nproj[m]
            nact = (nhalf + nhalf * jnp.tanh(nhalf)).astype(BF16)
            nmixed = dot_nn(nact, nout_v[...]) + bias_v[3:4, :]
            fin[m] = (node_v[m].astype(F32) + normed(nmixed, gain_v[1:2, :])).astype(BF16)
            pool[col * members + m] = fin[m, pl.ds(pl.multiple_of(col * rows, rows), rows), :]
            for d in range(peers - 1):
                fin_to(m, d).start()
            return carry

        lax.fori_loop(0, members, one_member, 0)

        def await_fin(m, carry):
            for d in range(peers - 1):
                fin_to(m, d).wait_recv()
            return carry

        lax.fori_loop(0, members, await_fin, 0)
        count = members * peers
        total = jnp.zeros((rows, width), F32)
        for i in range(count):
            total = total + pool[i].astype(F32)
        centre = total / count
        square = jnp.zeros((rows, width), F32)
        for i in range(count):
            dev = pool[i].astype(F32) - centre
            square = square + dev * dev
        result[col, 0] = centre.astype(BF16)
        result[col, 1] = jnp.sqrt(square / count).astype(BF16)

        def res_to(d):
            return pltpu.make_async_remote_copy(
                src_ref=result.at[col], dst_ref=result.at[col],
                send_sem=res_ssem.at[d], recv_sem=res_rsem.at[d],
                device_id={"graph": me, "member": peer_ids[d]}, device_id_type=MESH)

        for d in range(peers - 1):
            res_to(d).start()
        for d in range(peers - 1):
            res_to(d).wait_recv()
        for x in range(peers):
            mean_ref[x * rows : (x + 1) * rows, :] = result[x, 0]
            spread_ref[x * rows : (x + 1) * rows, :] = result[x, 1]

        for p in range(near):
            ask(p).wait_send()

        def drain(m, carry):
            for p in range(near):
                rows_to(m, p).wait_send()
            for d in range(peers - 1):
                fin_to(m, d).wait_send()
            return carry

        lax.fori_loop(0, members, drain, 0)
        for d in range(peers - 1):
            res_to(d).wait_send()

    return kernel


def local(node_latents, edge_latents, neighbours, edge_source, edge_dest, edge_count,
          edge_in, edge_out, node_in, node_out, biases, gains):
    members, blk, width = node_latents.shape
    slots = edge_source.shape[1]
    nbrs = neighbours.shape[1]
    groups = lax.axis_size("graph")
    peers = lax.axis_size("member")
    near = len(OFFSETS)
    halo = near * CAP
    rows = blk // peers
    vm = pltpu.VMEM
    dma = pltpu.SemaphoreType.DMA
    scratch = [
        vm((members, blk, width), BF16), vm((slots, width), BF16), vm((3, width, width), BF16),
        vm((width, width), BF16), vm((2, width, width), BF16), vm((width, width), BF16),
        vm((4, width), F32), vm((2, width), F32),
        vm((1, slots), jnp.int32), vm((1, slots), jnp.int32),
        pltpu.SMEM((1, nbrs), jnp.int32), pltpu.SMEM((1,), jnp.int32),
        vm((near, 8, blk), F32), vm((near, 8, blk), F32),
        vm((members, 4 * blk, width), BF16), vm((members, halo, width), BF16),
        vm((slots, 4 * blk), BF16), vm((slots, width), F32), vm((members, blk, width), F32),
        vm((blk, slots), BF16), vm((members, blk, width), BF16), vm((members * peers, rows, width), BF16),
        vm((peers, 2, rows, width), BF16),
        dma((15,)), dma((near,)), dma((near,)), dma((members, near)), dma((members, near)),
        dma((members, peers - 1)), dma((members, peers - 1)), dma((peers - 1,)), dma((peers - 1,)),
    ]
    out = jax.ShapeDtypeStruct((blk, width), BF16)
    return pl.pallas_call(
        make_kernel(groups, peers, members, blk, slots, width, nbrs, None),
        out_shape=(out, out),
        in_specs=[pl.BlockSpec(memory_space=pltpu.HBM)] * 12,
        out_specs=(pl.BlockSpec(memory_space=pltpu.VMEM),) * 2,
        scratch_shapes=scratch,
        compiler_params=pltpu.CompilerParams(
            collective_id=0, has_side_effects=True, vmem_limit_bytes=48 * 1024 * 1024
        ),
    )(node_latents, edge_latents, neighbours, edge_source, edge_dest, edge_count,
      edge_in, edge_out, node_in, node_out, biases, gains)


def solution(mesh):
    return jax.shard_map(
        local,
        mesh=mesh,
        in_specs=(
            P("member", "graph", None), P("graph", None), P("graph", None), P("graph", None),
            P("graph", None), P("graph"), P(), P(), P(), P(), P(), P(),
        ),
        out_specs=(P("graph", None), P("graph", None)),
        check_vma=False,
    )
```

```python
import jax
import jax.numpy as jnp
from jax import lax
from jax.experimental import pallas as pl
from jax.experimental.pallas import tpu as pltpu
from jax.sharding import PartitionSpec as P

RADIUS = 3
CAP = 32
EPS = 1e-05
MESH = pl.DeviceIdType.MESH
F32 = jnp.float32
BF16 = jnp.bfloat16
OFFSETS = tuple(range(1, RADIUS + 1)) + tuple(-r for r in range(1, RADIUS + 1))


def dot_nn(a, b):
    return lax.dot_general(a, b, (((1,), (0,)), ((), ())), preferred_element_type=F32)


def dot_nt(a, b):
    return lax.dot_general(a, b, (((1,), (1,)), ((), ())), preferred_element_type=F32)


def normed(values, gain):
    mean = jnp.mean(values, axis=-1, keepdims=True)
    cen = values - mean
    var = jnp.mean(cen * cen, axis=-1, keepdims=True)
    return cen * lax.rsqrt(var + EPS) * gain


def make_kernel(groups, peers, members, blk, slots, width, nbrs):
    near = len(OFFSETS)
    halo = near * CAP
    rows = blk // peers
    chunk = 256

    def kernel(
        node_hbm, edge_hbm, nbr_hbm, src_hbm, dst_hbm, cnt_ref,
        win_hbm, wout_hbm, nin_hbm, nout_hbm, bias_hbm, gain_hbm,
        mean_ref, spread_ref,
        node_v, edge_v, win_v, wout_v, nin_v, nout_v, bias_v, gain_v,
        src_v, dst_v, nbr_s,
        ask_out, ask_in, own, halo_in, outbox, hot, far_hot, eproj, pre, nproj, dhot, fin, pool, result,
        in_sems, ask_ssem, ask_rsem, row_ssem, row_rsem, fin_ssem, fin_rsem, res_ssem, res_rsem,
    ):
        me = lax.axis_index("graph")
        col = lax.axis_index("member")
        near_ids = [lax.rem(me + off + groups, groups) for off in OFFSETS]
        back_ids = [lax.rem(me - off + groups, groups) for off in OFFSETS]
        peer_ids = [lax.rem(col + d, peers) for d in range(1, peers)]

        barrier = pltpu.get_barrier_semaphore()
        for g in near_ids:
            pl.semaphore_signal(barrier, inc=1, device_id={"graph": g, "member": col}, device_id_type=MESH)
        for x in peer_ids:
            pl.semaphore_signal(barrier, inc=1, device_id={"graph": me, "member": x}, device_id_type=MESH)

        loads = [
            (src_hbm, src_v), (nbr_hbm, nbr_s), (dst_hbm, dst_v),
            (win_hbm.at[0, 1], win_v.at[1]), (node_hbm, node_v), (bias_hbm.at[0], bias_v), (gain_hbm.at[0], gain_v),
            (win_hbm.at[0, 2], win_v.at[2]), (win_hbm.at[0, 0], win_v.at[0]), (edge_hbm, edge_v),
            (nin_hbm.at[0, 0], nin_v.at[0]), (wout_hbm.at[0], wout_v),
            (nin_hbm.at[0, 1], nin_v.at[1]), (nout_hbm.at[0], nout_v),
        ]
        copies = [pltpu.make_async_copy(s, d, in_sems.at[i]) for i, (s, d) in enumerate(loads)]
        for c in copies:
            c.start()

        for c in copies[:3]:
            c.wait()
        lane_e = lax.broadcasted_iota(jnp.int32, (1, slots), 1)
        src = src_v[...]
        slot = src // blk
        node = src - slot * blk
        live = lane_e < cnt_ref[0]
        place = jnp.full((1, slots), near, jnp.int32)
        for s in range(nbrs):
            dist = lax.rem(nbr_s[0, s] - me + groups, groups)
            p = jnp.where(dist <= RADIUS, dist - 1, RADIUS - 1 + groups - dist)
            place = jnp.where(slot == s, p, place)
        sub8 = lax.broadcasted_iota(jnp.int32, (8, slots), 0)
        subn = lax.broadcasted_iota(jnp.int32, (blk, slots), 0)
        near_hot = jnp.where((sub8 == place) & live, 1.0, 0.0).astype(BF16)
        node_hot = jnp.where(subn == node, 1.0, 0.0).astype(BF16)
        used = jnp.where(dot_nt(near_hot, node_hot) > 0.5, 1.0, 0.0)
        sq_r = lax.broadcasted_iota(jnp.int32, (blk, blk), 0)
        sq_c = lax.broadcasted_iota(jnp.int32, (blk, blk), 1)
        before = jnp.where(sq_r < sq_c, 1.0, 0.0).astype(BF16)
        rank = jnp.where(used > 0.5, dot_nn(used.astype(BF16), before), 1000.0)
        for p in range(near):
            ask_out[p] = jnp.broadcast_to(rank[p : p + 1, :], (8, blk))
        capf = lax.broadcasted_iota(jnp.int32, (CAP, blk), 0).astype(F32)
        mine = jnp.concatenate(
            [jnp.where(capf == rank[p : p + 1, :], 1.0, 0.0) for p in range(near)], axis=0
        ).astype(BF16)

        for c in copies[3:7]:
            c.wait()

        def project(m, carry):
            part = dot_nn(node_v[m], win_v[1])
            own[m, 0:blk, :] = (0.5 * part).astype(BF16)
            return carry

        lax.fori_loop(0, members, project, 0)

        pl.semaphore_wait(barrier, near + peers - 1)

        def ask(p):
            return pltpu.make_async_remote_copy(
                src_ref=ask_out.at[p], dst_ref=ask_in.at[p], send_sem=ask_ssem.at[p], recv_sem=ask_rsem.at[p],
                device_id={"graph": near_ids[p], "member": col}, device_id_type=MESH)

        for p in range(near):
            ask(p).start()

        eye = jnp.where(sq_r == sq_c, 1.0, 0.0).astype(BF16)
        lane_n = sq_c.astype(F32)
        near_of = (lax.broadcasted_iota(jnp.int32, (blk, 2 * blk), 1) // CAP).astype(F32)
        dst = dst_v[...]
        for j in range(slots // blk):
            part = slice(j * blk, (j + 1) * blk)

            def column(row, n):
                return dot_nt(eye, jnp.broadcast_to(row[:, part].astype(F32), (n, blk)).astype(BF16))

            node_c = column(node, blk)
            dst_c = column(dst, blk)
            place_c = column(place, 2 * blk)
            one = jnp.where(node_c == lane_n, 1.0, 0.0)
            hot[part, 0:blk] = jnp.where(place_c[:, 0:blk] == float(near), one, 0.0).astype(BF16)
            hot[part, blk : 2 * blk] = jnp.where(dst_c == lane_n, 1.0, 0.0).astype(BF16)
            pick = dot_nt(one.astype(BF16), mine)
            pick = jnp.concatenate([pick, jnp.zeros((blk, 2 * blk - halo), F32)], axis=1)
            far_hot[part, :] = jnp.where(place_c == near_of, pick, 0.0).astype(BF16)
        dhot[...] = jnp.where((subn == dst) & live, 1.0, 0.0).astype(BF16)

        for c in copies[7:10]:
            c.wait()

        def project_receivers(m, carry):
            own[m, blk : 2 * blk, :] = (0.5 * dot_nn(node_v[m], win_v[2])).astype(BF16)
            halo_in[m, halo:, :] = jnp.zeros((2 * blk - halo, width), BF16)
            return carry

        lax.fori_loop(0, members, project_receivers, 0)

        def project_edges(j, carry):
            part = pl.ds(pl.multiple_of(j * chunk, chunk), chunk)
            eproj[part, :] = 0.5 * (dot_nn(edge_v[part, :], win_v[0]) + bias_v[0:1, :])
            return carry

        lax.fori_loop(0, slots // chunk, project_edges, 0)

        for p in range(near):
            ask(p).wait_recv()
        theirs = jnp.concatenate(
            [jnp.where(capf == ask_in[p, 0:1, :], 1.0, 0.0) for p in range(near)], axis=0
        ).astype(BF16)

        def rows_to(m, p):
            return pltpu.make_async_remote_copy(
                src_ref=outbox.at[m, pl.ds(p * CAP, CAP), :],
                dst_ref=halo_in.at[m, pl.ds(p * CAP, CAP), :],
                send_sem=row_ssem.at[m, p], recv_sem=row_rsem.at[m, p],
                device_id={"graph": back_ids[p], "member": col}, device_id_type=MESH)

        def select(m, carry):
            outbox[m] = dot_nn(theirs, own[m, 0:blk, :]).astype(BF16)
            for p in range(near):
                rows_to(m, p).start()
            return carry

        lax.fori_loop(0, members, select, 0)

        for c in copies[10:]:
            c.wait()

        def project_nodes(m, carry):
            nproj[m] = 0.5 * (dot_nn(node_v[m], nin_v[0]) + bias_v[2:3, :])
            return carry

        lax.fori_loop(0, members, project_nodes, 0)

        def precompute(m, carry):
            for j in range(slots // chunk):
                part = slice(j * chunk, (j + 1) * chunk)
                pre[m, part, :] = eproj[part, :] + dot_nn(hot[part, :], own[m])
            return carry

        lax.fori_loop(0, members, precompute, 0)

        def fin_to(m, d):
            return pltpu.make_async_remote_copy(
                src_ref=fin.at[m, pl.ds(pl.multiple_of(peer_ids[d] * rows, rows), rows), :],
                dst_ref=pool.at[col * members + m],
                send_sem=fin_ssem.at[m, d], recv_sem=fin_rsem.at[m, d],
                device_id={"graph": me, "member": peer_ids[d]}, device_id_type=MESH)

        def one_member(m, carry):
            for p in range(near):
                rows_to(m, p).wait_recv()
            half = pre[m] + dot_nn(far_hot[...], halo_in[m])
            act = (half + half * jnp.tanh(half)).astype(BF16)
            mixed = dot_nn(act, wout_v[...]) + bias_v[1:2, :]
            new = (edge_v[...].astype(F32) + normed(mixed, gain_v[0:1, :])).astype(BF16)
            total = dot_nn(dhot[...], new)
            nhalf = 0.5 * dot_nn(total.astype(BF16), nin_v[1]) + nproj[m]
            nact = (nhalf + nhalf * jnp.tanh(nhalf)).astype(BF16)
            nmixed = dot_nn(nact, nout_v[...]) + bias_v[3:4, :]
            fin[m] = (node_v[m].astype(F32) + normed(nmixed, gain_v[1:2, :])).astype(BF16)
            pool[col * members + m] = fin[m, pl.ds(pl.multiple_of(col * rows, rows), rows), :]
            for d in range(peers - 1):
                fin_to(m, d).start()
            return carry

        lax.fori_loop(0, members, one_member, 0)

        def await_fin(m, carry):
            for d in range(peers - 1):
                fin_to(m, d).wait_recv()
            return carry

        lax.fori_loop(0, members, await_fin, 0)
        count = members * peers
        total = jnp.zeros((rows, width), F32)
        for i in range(count):
            total = total + pool[i].astype(F32)
        centre = total / count
        square = jnp.zeros((rows, width), F32)
        for i in range(count):
            dev = pool[i].astype(F32) - centre
            square = square + dev * dev
        result[col, 0] = centre.astype(BF16)
        result[col, 1] = jnp.sqrt(square / count).astype(BF16)

        def res_to(d):
            return pltpu.make_async_remote_copy(
                src_ref=result.at[col], dst_ref=result.at[col],
                send_sem=res_ssem.at[d], recv_sem=res_rsem.at[d],
                device_id={"graph": me, "member": peer_ids[d]}, device_id_type=MESH)

        for d in range(peers - 1):
            res_to(d).start()
        for d in range(peers - 1):
            res_to(d).wait_recv()
        for x in range(peers):
            mean_ref[x * rows : (x + 1) * rows, :] = result[x, 0]
            spread_ref[x * rows : (x + 1) * rows, :] = result[x, 1]

        for p in range(near):
            ask(p).wait_send()

        def drain(m, carry):
            for p in range(near):
                rows_to(m, p).wait_send()
            for d in range(peers - 1):
                fin_to(m, d).wait_send()
            return carry

        lax.fori_loop(0, members, drain, 0)
        for d in range(peers - 1):
            res_to(d).wait_send()

    return kernel


def local(node_latents, edge_latents, neighbours, edge_source, edge_dest, edge_count,
          edge_in, edge_out, node_in, node_out, biases, gains):
    members, blk, width = node_latents.shape
    slots = edge_source.shape[1]
    nbrs = neighbours.shape[1]
    groups = lax.axis_size("graph")
    peers = lax.axis_size("member")
    near = len(OFFSETS)
    halo = near * CAP
    rows = blk // peers
    vm = pltpu.VMEM
    dma = pltpu.SemaphoreType.DMA
    scratch = [
        vm((members, blk, width), BF16), vm((slots, width), BF16), vm((3, width, width), BF16),
        vm((width, width), BF16), vm((2, width, width), BF16), vm((width, width), BF16),
        vm((4, width), F32), vm((2, width), F32),
        vm((1, slots), jnp.int32), vm((1, slots), jnp.int32),
        pltpu.SMEM((1, nbrs), jnp.int32),
        vm((near, 8, blk), F32), vm((near, 8, blk), F32),
        vm((members, 2 * blk, width), BF16), vm((members, 2 * blk, width), BF16), vm((members, halo, width), BF16),
        vm((slots, 2 * blk), BF16), vm((slots, 2 * blk), BF16), vm((slots, width), F32), vm((members, slots, width), F32), vm((members, blk, width), F32),
        vm((blk, slots), BF16), vm((members, blk, width), BF16), vm((members * peers, rows, width), BF16),
        vm((peers, 2, rows, width), BF16),
        dma((14,)), dma((near,)), dma((near,)), dma((members, near)), dma((members, near)),
        dma((members, peers - 1)), dma((members, peers - 1)), dma((peers - 1,)), dma((peers - 1,)),
    ]
    out = jax.ShapeDtypeStruct((blk, width), BF16)
    args = [node_latents, edge_latents, neighbours, edge_source, edge_dest, edge_count,
            edge_in, edge_out, node_in, node_out, biases, gains]
    specs = [pl.BlockSpec(memory_space=pltpu.HBM)] * len(args)
    specs[5] = pl.BlockSpec(memory_space=pltpu.SMEM)
    args = [a if i == 5 else pltpu.with_memory_space_constraint(a, pltpu.HBM) for i, a in enumerate(args)]
    return pl.pallas_call(
        make_kernel(groups, peers, members, blk, slots, width, nbrs),
        out_shape=(out, out),
        in_specs=specs,
        out_specs=(pl.BlockSpec(memory_space=pltpu.VMEM),) * 2,
        scratch_shapes=scratch,
        compiler_params=pltpu.CompilerParams(
            collective_id=0, has_side_effects=True, vmem_limit_bytes=52 * 1024 * 1024
        ),
    )(*args)


def solution(mesh):
    return jax.shard_map(
        local,
        mesh=mesh,
        in_specs=(
            P("member", "graph", None), P("graph", None), P("graph", None), P("graph", None),
            P("graph", None), P("graph"), P(), P(), P(), P(), P(), P(),
        ),
        out_specs=(P("graph", None), P("graph", None)),
        check_vma=False,
    )
```

```python
import jax
import jax.numpy as jnp
from jax import lax
from jax.experimental import pallas as pl
from jax.experimental.pallas import tpu as pltpu
from jax.sharding import PartitionSpec as P

RADIUS = 3
CAP = 32
EPS = 1e-05
PIECES = 2
MESH = pl.DeviceIdType.MESH
F32 = jnp.float32
BF16 = jnp.bfloat16
OFFSETS = tuple(range(1, RADIUS + 1)) + tuple(-r for r in range(1, RADIUS + 1))

FAR_FIRST = (2, 5, 1, 4, 0, 3)


def FAR_PEERS(peers):
    return sorted(range(1, peers), key=lambda d: -min(d, peers - d))


def dot_nn(a, b):
    return lax.dot_general(a, b, (((1,), (0,)), ((), ())), preferred_element_type=F32)


def dot_nt(a, b):
    return lax.dot_general(a, b, (((1,), (1,)), ((), ())), preferred_element_type=F32)


def normed(values, gain):
    mean = jnp.mean(values, axis=-1, keepdims=True)
    cen = values - mean
    var = jnp.mean(cen * cen, axis=-1, keepdims=True)
    return cen * lax.rsqrt(var + EPS) * gain


def make_kernel(groups, peers, members, blk, slots, width, nbrs):
    near = len(OFFSETS)
    halo = near * CAP
    rows = blk // peers
    piece = rows // PIECES

    def kernel(
        node_hbm, edge_hbm, nbr_hbm, src_hbm, dst_hbm, cnt_ref,
        win_hbm, wout_hbm, nin_hbm, nout_hbm, bias_hbm, gain_hbm,
        both_ref,
        node_v, edge_v, win_v, wout_v, nin_v, nout_v, bias_v, gain_v,
        src_v, dst_v, nbr_s,
        ask_out, ask_in, own, halo_in, outbox, hot, far_hot, eproj, pre, nproj, dhot, fin, pool, result,
        in_sems, ask_sems, row_ssem, row_rsem, fin_ssem, fin_rsem, res_ssem, res_rsem,
    ):
        me = lax.axis_index("graph")
        col = lax.axis_index("member")
        near_ids = [lax.rem(me + off + groups, groups) for off in OFFSETS]
        back_ids = [lax.rem(me - off + groups, groups) for off in OFFSETS]
        peer_ids = [lax.rem(col + d, peers) for d in FAR_PEERS(peers)]

        def load(i, s, d):
            return pltpu.make_async_copy(s, d, in_sems.at[i])

        loads = [
            (src_hbm, src_v), (nbr_hbm, nbr_s), (dst_hbm, dst_v),
            (win_hbm.at[0, 1], win_v.at[1]), (node_hbm, node_v), (bias_hbm.at[0], bias_v), (gain_hbm.at[0], gain_v),
            (win_hbm.at[0, 2], win_v.at[2]), (win_hbm.at[0, 0], win_v.at[0]), (edge_hbm, edge_v),
            (nin_hbm.at[0, 0], nin_v.at[0]), (wout_hbm.at[0], wout_v),
            (nin_hbm.at[0, 1], nin_v.at[1]), (nout_hbm.at[0], nout_v),
        ]
        copies = [load(i, s, d) for i, (s, d) in enumerate(loads)]
        for c in copies[:2]:
            c.start()
        barrier = pltpu.get_barrier_semaphore()
        for g in near_ids:
            pl.semaphore_signal(barrier, inc=1, device_id={"graph": g, "member": col}, device_id_type=MESH)
        for x in peer_ids:
            pl.semaphore_signal(barrier, inc=1, device_id={"graph": me, "member": x}, device_id_type=MESH)
        for c in copies[2:]:
            c.start()

        with jax.named_scope("s01_load"):
            for c in copies[:2]:
                c.wait()
        with jax.named_scope("s02_rank"):
            lane_e = lax.broadcasted_iota(jnp.int32, (1, slots), 1)
            src = src_v[...]
            slot = src // blk
            node = src - slot * blk
            live = lane_e < cnt_ref[0]
            place = jnp.full((1, slots), near, jnp.int32)
            for s in range(nbrs):
                dist = lax.rem(nbr_s[0, s] - me + groups, groups)
                p = jnp.where(dist <= RADIUS, dist - 1, RADIUS - 1 + groups - dist)
                place = jnp.where(slot == s, p, place)
            sub8 = lax.broadcasted_iota(jnp.int32, (8, slots), 0)
            subn = lax.broadcasted_iota(jnp.int32, (blk, slots), 0)
            near_hot = jnp.where((sub8 == place) & live, 1.0, 0.0).astype(BF16)
            node_hot = jnp.where(subn == node, 1.0, 0.0).astype(BF16)
            used = jnp.where(dot_nt(near_hot, node_hot) > 0.5, 1.0, 0.0)
            sq_r = lax.broadcasted_iota(jnp.int32, (blk, blk), 0)
            sq_c = lax.broadcasted_iota(jnp.int32, (blk, blk), 1)
            before = jnp.where(sq_r < sq_c, 1.0, 0.0).astype(BF16)
            rank = jnp.where(used > 0.5, dot_nn(used.astype(BF16), before), 1000.0)
            for p in range(near):
                ask_out[p] = jnp.broadcast_to(rank[p : p + 1, :], (8, blk))
            capf = lax.broadcasted_iota(jnp.int32, (CAP, blk), 0).astype(F32)
            mine = jnp.concatenate(
                [jnp.where(capf == rank[p : p + 1, :], 1.0, 0.0) for p in range(near)], axis=0
            ).astype(BF16)

        with jax.named_scope("s03_barrier"):
            pl.semaphore_wait(barrier, near + peers - 1)

        def ask(p):
            return pltpu.make_async_remote_copy(
                src_ref=ask_out.at[p], dst_ref=ask_in.at[p], send_sem=ask_sems.at[0], recv_sem=ask_sems.at[1],
                device_id={"graph": near_ids[p], "member": col}, device_id_type=MESH)

        for p in FAR_FIRST:
            ask(p).start()

        with jax.named_scope("s04_project"):
            for c in copies[2:5]:
                c.wait()
            part = (0.5 * dot_nn(node_v[...], win_v[1])).astype(BF16)
            for m in range(members):
                own[m, 0:blk, :] = part[m * blk : (m + 1) * blk, :]

        with jax.named_scope("s05_hot"):
            eye = jnp.where(sq_r == sq_c, 1.0, 0.0).astype(BF16)
            lane_n = sq_c.astype(F32)
            near_of = (lax.broadcasted_iota(jnp.int32, (blk, 2 * blk), 1) // CAP).astype(F32)
            dst = dst_v[...]
            for j in range(slots // blk):
                part = slice(j * blk, (j + 1) * blk)

                def column(row, n):
                    return dot_nt(eye, jnp.broadcast_to(row[:, part].astype(F32), (n, blk)).astype(BF16))

                node_c = column(node, blk)
                dst_c = column(dst, blk)
                place_c = column(place, 2 * blk)
                one = jnp.where(node_c == lane_n, 1.0, 0.0)
                hot[part, 0:blk] = jnp.where(place_c[:, 0:blk] == float(near), one, 0.0).astype(BF16)
                hot[part, blk : 2 * blk] = jnp.where(dst_c == lane_n, 1.0, 0.0).astype(BF16)
                pick = dot_nt(one.astype(BF16), mine)
                pick = jnp.concatenate([pick, jnp.zeros((blk, 2 * blk - halo), F32)], axis=1)
                far_hot[part, :] = jnp.where(place_c == near_of, pick, 0.0).astype(BF16)
            dhot[...] = jnp.where((subn == dst) & live, 1.0, 0.0).astype(BF16)

        with jax.named_scope("s06_askwait"):
            pltpu.make_async_copy(ask_in, ask_in, ask_sems.at[1]).wait()

        def rows_to(m, p):
            return pltpu.make_async_remote_copy(
                src_ref=outbox.at[m, pl.ds(p * CAP, CAP), :],
                dst_ref=halo_in.at[m, pl.ds(p * CAP, CAP), :],
                send_sem=row_ssem, recv_sem=row_rsem.at[m],
                device_id={"graph": back_ids[p], "member": col}, device_id_type=MESH)

        with jax.named_scope("s07_select"):
            theirs = jnp.concatenate(
                [jnp.where(capf == ask_in[p, 0:1, :], 1.0, 0.0) for p in range(near)], axis=0
            ).astype(BF16)

            def select(m, carry):
                outbox[m] = dot_nn(theirs, own[m, 0:blk, :]).astype(BF16)
                for p in FAR_FIRST:
                    rows_to(m, p).start()
                return carry

            lax.fori_loop(0, members, select, 0)

        with jax.named_scope("s08_recv"):
            for c in copies[5:8]:
                c.wait()
            part = (0.5 * dot_nn(node_v[...], win_v[2])).astype(BF16)
            for m in range(members):
                own[m, blk : 2 * blk, :] = part[m * blk : (m + 1) * blk, :]
                halo_in[m, halo:, :] = jnp.zeros((2 * blk - halo, width), BF16)
        with jax.named_scope("s09_eproj"):
            for c in copies[8:10]:
                c.wait()
            eproj[...] = 0.5 * (dot_nn(edge_v[...], win_v[0]) + bias_v[0:1, :])
        with jax.named_scope("s10_pre"):

            def precompute(m, carry):
                pre[m] = eproj[...] + dot_nn(hot[...], own[m])
                return carry

            lax.fori_loop(0, members, precompute, 0)
        with jax.named_scope("s11_nodes"):
            for c in copies[10:]:
                c.wait()
            nproj[...] = 0.5 * (dot_nn(node_v[...], nin_v[0]) + bias_v[2:3, :])

        def fin_to(m, d, h):
            at = pl.multiple_of(peer_ids[d] * rows + h * piece, piece)
            return pltpu.make_async_remote_copy(
                src_ref=fin.at[m, pl.ds(at, piece), :],
                dst_ref=pool.at[h, col * members + m],
                send_sem=fin_ssem, recv_sem=fin_rsem.at[h],
                device_id={"graph": me, "member": peer_ids[d]}, device_id_type=MESH)

        def one_member(m, carry):
            with jax.named_scope("m1_rowwait"):
                arrived = halo_in.at[m, pl.ds(0, halo), :]
                pltpu.make_async_copy(arrived, arrived, row_rsem.at[m]).wait()
            with jax.named_scope("m2_edge"):
                half = pre[m] + dot_nn(far_hot[...], halo_in[m])
                act = (half + half * jnp.tanh(half)).astype(BF16)
                mixed = dot_nn(act, wout_v[...]) + bias_v[1:2, :]
                new = (edge_v[...].astype(F32) + normed(mixed, gain_v[0:1, :])).astype(BF16)
                total = dot_nn(dhot[...], new)
            with jax.named_scope("m3_node"):
                mine_at = pl.ds(pl.multiple_of(m * blk, blk), blk)
                nhalf = 0.5 * dot_nn(total.astype(BF16), nin_v[1]) + nproj[mine_at, :]
                nact = (nhalf + nhalf * jnp.tanh(nhalf)).astype(BF16)
                nmixed = dot_nn(nact, nout_v[...]) + bias_v[3:4, :]
                fin[m] = (node_v[mine_at, :].astype(F32) + normed(nmixed, gain_v[1:2, :])).astype(BF16)
                for h in range(PIECES):
                    for d in range(peers - 1):
                        fin_to(m, d, h).start()
                for h in range(PIECES):
                    at = pl.multiple_of(col * rows + h * piece, piece)
                    pool[h, col * members + m] = fin[m, pl.ds(at, piece), :]
            return carry

        lax.fori_loop(0, members, one_member, 0)

        with jax.named_scope("t0_drain"):
            pltpu.make_async_copy(ask_out, ask_out, ask_sems.at[0]).wait()
            pltpu.make_async_copy(outbox, outbox, row_ssem).wait()

        def res_to(d, h):
            return pltpu.make_async_remote_copy(
                src_ref=result.at[h, col], dst_ref=result.at[h, col],
                send_sem=res_ssem, recv_sem=res_rsem,
                device_id={"graph": me, "member": peer_ids[d]}, device_id_type=MESH)

        count = members * peers
        for h in range(PIECES):
            others = pool.at[h, pl.ds(0, members * (peers - 1))]
            with jax.named_scope("t1_finwait"):
                pltpu.make_async_copy(others, others, fin_rsem.at[h]).wait()
            with jax.named_scope("t2_final"):
                total = jnp.zeros((piece, width), F32)
                for i in range(count):
                    total = total + pool[h, i].astype(F32)
                centre = total / count
                square = jnp.zeros((piece, width), F32)
                for i in range(count):
                    dev = pool[h, i].astype(F32) - centre
                    square = square + dev * dev
                result[h, col, 0] = centre.astype(BF16)
                result[h, col, 1] = jnp.sqrt(square / count).astype(BF16)
                for d in range(peers - 1):
                    res_to(d, h).start()
        all_fin = pool.at[:, pl.ds(0, members * (peers - 1))]
        three = result.at[:, pl.ds(0, peers - 1)]
        with jax.named_scope("t3_reswait"):
            pltpu.make_async_copy(all_fin, all_fin, fin_ssem).wait()
            pltpu.make_async_copy(three, three, res_rsem).wait()
        with jax.named_scope("t4_out"):
            for x in range(peers):
                for h in range(PIECES):
                    at = slice(x * rows + h * piece, x * rows + (h + 1) * piece)
                    both_ref[0, at, :] = result[h, x, 0]
                    both_ref[1, at, :] = result[h, x, 1]
            pltpu.make_async_copy(three, three, res_ssem).wait()

    return kernel


def local(node_latents, edge_latents, neighbours, edge_source, edge_dest, edge_count,
          edge_in, edge_out, node_in, node_out, biases, gains):
    members, blk, width = node_latents.shape
    slots = edge_source.shape[1]
    nbrs = neighbours.shape[1]
    groups = lax.axis_size("graph")
    peers = lax.axis_size("member")
    near = len(OFFSETS)
    halo = near * CAP
    rows = blk // peers
    piece = rows // PIECES
    vm = pltpu.VMEM
    dma = pltpu.SemaphoreType.DMA
    scratch = [
        vm((members * blk, width), BF16), vm((slots, width), BF16), vm((3, width, width), BF16),
        vm((width, width), BF16), vm((2, width, width), BF16), vm((width, width), BF16),
        vm((4, width), F32), vm((2, width), F32),
        vm((1, slots), jnp.int32), vm((1, slots), jnp.int32),
        pltpu.SMEM((1, nbrs), jnp.int32),
        vm((near, 8, blk), F32), vm((near, 8, blk), F32),
        vm((members, 2 * blk, width), BF16), vm((members, 2 * blk, width), BF16), vm((members, halo, width), BF16),
        vm((slots, 2 * blk), BF16), vm((slots, 2 * blk), BF16), vm((slots, width), F32), vm((members, slots, width), F32), vm((members * blk, width), F32),
        vm((blk, slots), BF16), vm((members, blk, width), BF16), vm((PIECES, members * peers, piece, width), BF16),
        vm((PIECES, peers, 2, piece, width), BF16),
        dma((14,)), dma((2,)), dma(()), dma((members,)), dma(()), dma((PIECES,)), dma(()), dma(()),
    ]
    out = jax.ShapeDtypeStruct((blk, width), BF16)
    args = [node_latents.reshape(members * blk, width), edge_latents, neighbours, edge_source, edge_dest, edge_count,
            edge_in, edge_out, node_in, node_out, biases, gains]
    specs = [pl.BlockSpec(memory_space=pltpu.HBM)] * len(args)
    specs[5] = pl.BlockSpec(memory_space=pltpu.SMEM)
    args = [a if i == 5 else pltpu.with_memory_space_constraint(a, pltpu.HBM) for i, a in enumerate(args)]
    both = pl.pallas_call(
        make_kernel(groups, peers, members, blk, slots, width, nbrs),
        out_shape=jax.ShapeDtypeStruct((2, blk, width), BF16),
        in_specs=specs,
        out_specs=pl.BlockSpec(memory_space=pltpu.VMEM),
        scratch_shapes=scratch,
        compiler_params=pltpu.CompilerParams(
            collective_id=0, has_side_effects=True, vmem_limit_bytes=52 * 1024 * 1024
        ),
    )(*args)
    return both[0], both[1]


def solution(mesh):
    return jax.shard_map(
        local,
        mesh=mesh,
        in_specs=(
            P("member", "graph", None), P("graph", None), P("graph", None), P("graph", None),
            P("graph", None), P("graph"), P(), P(), P(), P(), P(), P(),
        ),
        out_specs=(P("graph", None), P("graph", None)),
        check_vma=False,
    )
```

```python
import jax
import jax.numpy as jnp
from jax import lax
from jax.experimental import pallas as pl
from jax.experimental.pallas import tpu as pltpu
from jax.sharding import PartitionSpec as P

RADIUS = 3
CAP = 32
EPS = 1e-05
PIECES = 2
RELAY = 15
MESH = pl.DeviceIdType.MESH
F32 = jnp.float32
BF16 = jnp.bfloat16
OFFSETS = tuple(range(1, RADIUS + 1)) + tuple(-r for r in range(1, RADIUS + 1))

FAR_FIRST = (2, 5, 1, 4, 0, 3)


def FAR_PEERS(peers):
    return sorted(range(1, peers), key=lambda d: -min(d, peers - d))


def dot_nn(a, b):
    return lax.dot_general(a, b, (((1,), (0,)), ((), ())), preferred_element_type=F32)


def dot_nt(a, b):
    return lax.dot_general(a, b, (((1,), (1,)), ((), ())), preferred_element_type=F32)


def normed(values, gain):
    mean = jnp.mean(values, axis=-1, keepdims=True)
    cen = values - mean
    var = jnp.mean(cen * cen, axis=-1, keepdims=True)
    return cen * lax.rsqrt(var + EPS) * gain


def make_kernel(groups, peers, members, blk, slots, width, nbrs):
    near = len(OFFSETS)
    halo = near * CAP
    rows = blk // peers
    piece = rows // PIECES

    def kernel(
        node_hbm, edge_hbm, nbr_hbm, src_hbm, dst_hbm, cnt_ref,
        win_hbm, wout_hbm, nin_hbm, nout_hbm, bias_hbm, gain_hbm,
        both_ref,
        node_v, edge_v, win_v, wout_v, nin_v, nout_v, bias_v, gain_v,
        src_v, dst_v, nbr_s,
        ask_out, ask_in, relay_in, own, halo_in, outbox, hot, far_hot, eproj, pre, nproj, dhot, fin, pool, result,
        in_sems, ask_ssem, ask_rsem, relay_ssem, relay_rsem, row_ssem, row_rsem, fin_ssem, fin_rsem, res_ssem, res_rsem,
    ):
        me = lax.axis_index("graph")
        col = lax.axis_index("member")
        near_ids = [lax.rem(me + off + groups, groups) for off in OFFSETS]
        back_ids = [lax.rem(me - off + groups, groups) for off in OFFSETS]
        peer_ids = [lax.rem(col + d, peers) for d in FAR_PEERS(peers)]

        def load(i, s, d):
            return pltpu.make_async_copy(s, d, in_sems.at[i])

        loads = [
            (src_hbm, src_v), (nbr_hbm, nbr_s), (dst_hbm, dst_v),
            (win_hbm.at[0, 1], win_v.at[1]), (node_hbm, node_v), (bias_hbm.at[0], bias_v), (gain_hbm.at[0], gain_v),
            (win_hbm.at[0, 2], win_v.at[2]), (win_hbm.at[0, 0], win_v.at[0]), (edge_hbm, edge_v),
            (nin_hbm.at[0, 0], nin_v.at[0]), (wout_hbm.at[0], wout_v),
            (nin_hbm.at[0, 1], nin_v.at[1]), (nout_hbm.at[0], nout_v),
        ]
        copies = [load(i, s, d) for i, (s, d) in enumerate(loads)]
        for c in copies[:2]:
            c.start()
        is_first, is_last, is_relay = me < RADIUS, me >= groups - RADIUS, me == RELAY

        barrier = pltpu.get_barrier_semaphore()

        def greet(g, x):
            pl.semaphore_signal(barrier, inc=1, device_id={"graph": g, "member": x}, device_id_type=MESH)

        pl.when(is_last)(lambda: greet(RELAY, col))
        for p in FAR_FIRST:
            if OFFSETS[p] > 0:
                greet(back_ids[p], col)
            else:
                pl.when(me - OFFSETS[p] < groups)(lambda p=p: greet(back_ids[p], col))
        for x in peer_ids:
            greet(me, x)

        @pl.when(is_relay)
        def _():
            for e in range(RADIUS):
                greet(e, col)

        expected = near + peers - 1 + jnp.where(is_first, 1 + me - RADIUS, 0) + jnp.where(is_relay, RADIUS, 0)
        for c in copies[2:]:
            c.start()

        with jax.named_scope("s01_load"):
            for c in copies[:2]:
                c.wait()
        with jax.named_scope("s02_rank"):
            lane_e = lax.broadcasted_iota(jnp.int32, (1, slots), 1)
            src = src_v[...]
            slot = src // blk
            node = src - slot * blk
            live = lane_e < cnt_ref[0]
            place = jnp.full((1, slots), near, jnp.int32)
            for s in range(nbrs):
                dist = lax.rem(nbr_s[0, s] - me + groups, groups)
                p = jnp.where(dist <= RADIUS, dist - 1, RADIUS - 1 + groups - dist)
                place = jnp.where(slot == s, p, place)
            sub8 = lax.broadcasted_iota(jnp.int32, (8, slots), 0)
            subn = lax.broadcasted_iota(jnp.int32, (blk, slots), 0)
            near_hot = jnp.where((sub8 == place) & live, 1.0, 0.0).astype(BF16)
            node_hot = jnp.where(subn == node, 1.0, 0.0).astype(BF16)
            used = jnp.where(dot_nt(near_hot, node_hot) > 0.5, 1.0, 0.0)
            sq_r = lax.broadcasted_iota(jnp.int32, (blk, blk), 0)
            sq_c = lax.broadcasted_iota(jnp.int32, (blk, blk), 1)
            before = jnp.where(sq_r < sq_c, 1.0, 0.0).astype(BF16)
            rank = jnp.where(used > 0.5, dot_nn(used.astype(BF16), before), 1000.0)
            for p in range(near):
                ask_out[p] = jnp.broadcast_to(rank[p : p + 1, :], (8, blk))
            capf = lax.broadcasted_iota(jnp.int32, (CAP, blk), 0).astype(F32)
            mine = jnp.concatenate(
                [jnp.where(capf == rank[p : p + 1, :], 1.0, 0.0) for p in range(near)], axis=0
            ).astype(BF16)

        with jax.named_scope("s03_barrier"):
            pl.semaphore_wait(barrier, expected)

        def ask(p):
            return pltpu.make_async_remote_copy(
                src_ref=ask_out.at[p], dst_ref=ask_in.at[p], send_sem=ask_ssem, recv_sem=ask_rsem.at[p // RADIUS],
                device_id={"graph": near_ids[p], "member": col}, device_id_type=MESH)

        def ask_relay(p):
            return pltpu.make_async_remote_copy(
                src_ref=ask_out.at[p], dst_ref=relay_in.at[me * RADIUS + p - RADIUS],
                send_sem=ask_ssem, recv_sem=relay_rsem,
                device_id={"graph": RELAY, "member": col}, device_id_type=MESH)

        def forward(e, o):
            return pltpu.make_async_remote_copy(
                src_ref=relay_in.at[e * RADIUS + o - 1], dst_ref=ask_in.at[RADIUS + o - 1],
                send_sem=relay_ssem, recv_sem=ask_rsem.at[1],
                device_id={"graph": groups + e - o, "member": col}, device_id_type=MESH)

        for p in FAR_FIRST:
            if OFFSETS[p] > 0:
                ask(p).start()
            else:
                pl.when(me + OFFSETS[p] >= 0)(lambda p=p: ask(p).start())
                pl.when(me + OFFSETS[p] < 0)(lambda p=p: ask_relay(p).start())

        @pl.when(is_relay)
        def _():
            with jax.named_scope("s035_relay"):
                pltpu.make_async_copy(ask_out, ask_out, relay_rsem).wait()
                for e in range(RADIUS):
                    for o in range(e + 1, RADIUS + 1):
                        forward(e, o).start()

        with jax.named_scope("s04_project"):
            for c in copies[2:5]:
                c.wait()
            part = (0.5 * dot_nn(node_v[...], win_v[1])).astype(BF16)
            for m in range(members):
                own[m, 0:blk, :] = part[m * blk : (m + 1) * blk, :]

        with jax.named_scope("s05_hot"):
            eye = jnp.where(sq_r == sq_c, 1.0, 0.0).astype(BF16)
            lane_n = sq_c.astype(F32)
            near_of = (lax.broadcasted_iota(jnp.int32, (blk, 2 * blk), 1) // CAP).astype(F32)
            dst = dst_v[...]
            for j in range(slots // blk):
                part = slice(j * blk, (j + 1) * blk)

                def column(row, n):
                    return dot_nt(eye, jnp.broadcast_to(row[:, part].astype(F32), (n, blk)).astype(BF16))

                node_c = column(node, blk)
                dst_c = column(dst, blk)
                place_c = column(place, 2 * blk)
                one = jnp.where(node_c == lane_n, 1.0, 0.0)
                hot[part, 0:blk] = jnp.where(place_c[:, 0:blk] == float(near), one, 0.0).astype(BF16)
                hot[part, blk : 2 * blk] = jnp.where(dst_c == lane_n, 1.0, 0.0).astype(BF16)
                pick = dot_nt(one.astype(BF16), mine)
                pick = jnp.concatenate([pick, jnp.zeros((blk, 2 * blk - halo), F32)], axis=1)
                far_hot[part, :] = jnp.where(place_c == near_of, pick, 0.0).astype(BF16)
            dhot[...] = jnp.where((subn == dst) & live, 1.0, 0.0).astype(BF16)

        def rows_to(m, p):
            return pltpu.make_async_remote_copy(
                src_ref=outbox.at[m, pl.ds(p * CAP, CAP), :],
                dst_ref=halo_in.at[m, pl.ds(p * CAP, CAP), :],
                send_sem=row_ssem, recv_sem=row_rsem.at[m],
                device_id={"graph": back_ids[p], "member": col}, device_id_type=MESH)

        def serve(side):
            first = side * RADIUS
            with jax.named_scope("s06_askwait"):
                asks = ask_in.at[pl.ds(first, RADIUS)]
                pltpu.make_async_copy(asks, asks, ask_rsem.at[side]).wait()
            with jax.named_scope("s07_select"):
                theirs = jnp.concatenate(
                    [jnp.where(capf == ask_in[p, 0:1, :], 1.0, 0.0) for p in range(first, first + RADIUS)], axis=0
                ).astype(BF16)

                def select(m, carry):
                    outbox[m, first * CAP : (first + RADIUS) * CAP, :] = dot_nn(theirs, own[m, 0:blk, :]).astype(BF16)
                    for p in reversed(range(first, first + RADIUS)):
                        rows_to(m, p).start()
                    return carry

                lax.fori_loop(0, members, select, 0)

        def local_work():
            with jax.named_scope("s08_recv"):
                for c in copies[5:8]:
                    c.wait()
                part = (0.5 * dot_nn(node_v[...], win_v[2])).astype(BF16)
                for m in range(members):
                    own[m, blk : 2 * blk, :] = part[m * blk : (m + 1) * blk, :]
                    halo_in[m, halo:, :] = jnp.zeros((2 * blk - halo, width), BF16)
            with jax.named_scope("s09_eproj"):
                for c in copies[8:10]:
                    c.wait()
                eproj[...] = 0.5 * (dot_nn(edge_v[...], win_v[0]) + bias_v[0:1, :])
            with jax.named_scope("s10_pre"):

                def precompute(m, carry):
                    pre[m] = eproj[...] + dot_nn(hot[...], own[m])
                    return carry

                lax.fori_loop(0, members, precompute, 0)
            with jax.named_scope("s11_nodes"):
                for c in copies[10:]:
                    c.wait()
                nproj[...] = 0.5 * (dot_nn(node_v[...], nin_v[0]) + bias_v[2:3, :])

        serve(1)
        pl.when(is_first)(local_work)
        serve(0)
        pl.when(me >= RADIUS)(local_work)

        def fin_to(m, d, h):
            at = pl.multiple_of(peer_ids[d] * rows + h * piece, piece)
            return pltpu.make_async_remote_copy(
                src_ref=fin.at[m, pl.ds(at, piece), :],
                dst_ref=pool.at[h, col * members + m],
                send_sem=fin_ssem, recv_sem=fin_rsem.at[h],
                device_id={"graph": me, "member": peer_ids[d]}, device_id_type=MESH)

        def one_member(m, carry):
            with jax.named_scope("m1_rowwait"):
                arrived = halo_in.at[m, pl.ds(0, halo), :]
                pltpu.make_async_copy(arrived, arrived, row_rsem.at[m]).wait()
            with jax.named_scope("m2_edge"):
                half = pre[m] + dot_nn(far_hot[...], halo_in[m])
                act = (half + half * jnp.tanh(half)).astype(BF16)
                mixed = dot_nn(act, wout_v[...]) + bias_v[1:2, :]
                new = (edge_v[...].astype(F32) + normed(mixed, gain_v[0:1, :])).astype(BF16)
                total = dot_nn(dhot[...], new)
            with jax.named_scope("m3_node"):
                mine_at = pl.ds(pl.multiple_of(m * blk, blk), blk)
                nhalf = 0.5 * dot_nn(total.astype(BF16), nin_v[1]) + nproj[mine_at, :]
                nact = (nhalf + nhalf * jnp.tanh(nhalf)).astype(BF16)
                nmixed = dot_nn(nact, nout_v[...]) + bias_v[3:4, :]
                fin[m] = (node_v[mine_at, :].astype(F32) + normed(nmixed, gain_v[1:2, :])).astype(BF16)
                for h in range(PIECES):
                    for d in range(peers - 1):
                        fin_to(m, d, h).start()
                for h in range(PIECES):
                    at = pl.multiple_of(col * rows + h * piece, piece)
                    pool[h, col * members + m] = fin[m, pl.ds(at, piece), :]
            return carry

        lax.fori_loop(0, members, one_member, 0)

        with jax.named_scope("t0_drain"):
            pltpu.make_async_copy(ask_out, ask_out, ask_ssem).wait()

            @pl.when(is_relay)
            def _():
                pltpu.make_async_copy(ask_out, ask_out, relay_ssem).wait()

            pltpu.make_async_copy(outbox, outbox, row_ssem).wait()

        def res_to(d, h):
            return pltpu.make_async_remote_copy(
                src_ref=result.at[h, col], dst_ref=result.at[h, col],
                send_sem=res_ssem, recv_sem=res_rsem,
                device_id={"graph": me, "member": peer_ids[d]}, device_id_type=MESH)

        count = members * peers
        for h in range(PIECES):
            others = pool.at[h, pl.ds(0, members * (peers - 1))]
            with jax.named_scope("t1_finwait"):
                pltpu.make_async_copy(others, others, fin_rsem.at[h]).wait()
            with jax.named_scope("t2_final"):
                total = jnp.zeros((piece, width), F32)
                for i in range(count):
                    total = total + pool[h, i].astype(F32)
                centre = total / count
                square = jnp.zeros((piece, width), F32)
                for i in range(count):
                    dev = pool[h, i].astype(F32) - centre
                    square = square + dev * dev
                result[h, col, 0] = centre.astype(BF16)
                result[h, col, 1] = jnp.sqrt(square / count).astype(BF16)
                for d in range(peers - 1):
                    res_to(d, h).start()
        all_fin = pool.at[:, pl.ds(0, members * (peers - 1))]
        three = result.at[:, pl.ds(0, peers - 1)]
        with jax.named_scope("t3_reswait"):
            pltpu.make_async_copy(all_fin, all_fin, fin_ssem).wait()
            pltpu.make_async_copy(three, three, res_rsem).wait()
        with jax.named_scope("t4_out"):
            for x in range(peers):
                for h in range(PIECES):
                    at = slice(x * rows + h * piece, x * rows + (h + 1) * piece)
                    both_ref[0, at, :] = result[h, x, 0]
                    both_ref[1, at, :] = result[h, x, 1]
            pltpu.make_async_copy(three, three, res_ssem).wait()

    return kernel


def local(node_latents, edge_latents, neighbours, edge_source, edge_dest, edge_count,
          edge_in, edge_out, node_in, node_out, biases, gains):
    members, blk, width = node_latents.shape
    slots = edge_source.shape[1]
    nbrs = neighbours.shape[1]
    groups = lax.axis_size("graph")
    peers = lax.axis_size("member")
    near = len(OFFSETS)
    halo = near * CAP
    rows = blk // peers
    piece = rows // PIECES
    vm = pltpu.VMEM
    dma = pltpu.SemaphoreType.DMA
    scratch = [
        vm((members * blk, width), BF16), vm((slots, width), BF16), vm((3, width, width), BF16),
        vm((width, width), BF16), vm((2, width, width), BF16), vm((width, width), BF16),
        vm((4, width), F32), vm((2, width), F32),
        vm((1, slots), jnp.int32), vm((1, slots), jnp.int32),
        pltpu.SMEM((1, nbrs), jnp.int32),
        vm((near, 8, blk), F32), vm((near, 8, blk), F32), vm((RADIUS * RADIUS, 8, blk), F32),
        vm((members, 2 * blk, width), BF16), vm((members, 2 * blk, width), BF16), vm((members, halo, width), BF16),
        vm((slots, 2 * blk), BF16), vm((slots, 2 * blk), BF16), vm((slots, width), F32), vm((members, slots, width), F32), vm((members * blk, width), F32),
        vm((blk, slots), BF16), vm((members, blk, width), BF16), vm((PIECES, members * peers, piece, width), BF16),
        vm((PIECES, peers, 2, piece, width), BF16),
        dma((14,)), dma(()), dma((2,)), dma(()), dma(()), dma(()), dma((members,)), dma(()), dma((PIECES,)), dma(()), dma(()),
    ]
    out = jax.ShapeDtypeStruct((blk, width), BF16)
    args = [node_latents.reshape(members * blk, width), edge_latents, neighbours, edge_source, edge_dest, edge_count,
            edge_in, edge_out, node_in, node_out, biases, gains]
    specs = [pl.BlockSpec(memory_space=pltpu.HBM)] * len(args)
    specs[5] = pl.BlockSpec(memory_space=pltpu.SMEM)
    args = [a if i == 5 else pltpu.with_memory_space_constraint(a, pltpu.HBM) for i, a in enumerate(args)]
    both = pl.pallas_call(
        make_kernel(groups, peers, members, blk, slots, width, nbrs),
        out_shape=jax.ShapeDtypeStruct((2, blk, width), BF16),
        in_specs=specs,
        out_specs=pl.BlockSpec(memory_space=pltpu.VMEM),
        scratch_shapes=scratch,
        compiler_params=pltpu.CompilerParams(
            collective_id=0, has_side_effects=True, vmem_limit_bytes=52 * 1024 * 1024
        ),
    )(*args)
    return both[0], both[1]


def solution(mesh):
    return jax.shard_map(
        local,
        mesh=mesh,
        in_specs=(
            P("member", "graph", None), P("graph", None), P("graph", None), P("graph", None),
            P("graph", None), P("graph"), P(), P(), P(), P(), P(), P(),
        ),
        out_specs=(P("graph", None), P("graph", None)),
        check_vma=False,
    )
```
